128 devices in a mesh: wide: 32 (over z, y, x_hi), narrow: 4 (over x_lo, core).
Axes of the slice: x: 4 (x_hi: 2, x_lo: 2; x = x_hi * 2 + x_lo), y: 4, z: 4, core: 2. Of those that a mesh axis runs over, the one named last changes fastest.
Arguments:
- image_tower: bfloat16 [64, 2560, 1024], P('wide', 'narrow'), may hold values from -150 to 150
- text_tower: bfloat16 [163840, 1024], P(('wide', 'narrow')), may hold values from -150 to 150
- image_proj: bfloat16 [2, 1024, 768], replicated, may hold values from -1 to 1
- text_proj: bfloat16 [2, 1024, 768], replicated, may hold values from -1 to 1
- logit_scale: float32 [2], replicated, may hold values from 8 to 300
- pair_ids: int32 [163840], P(('wide', 'narrow')), may hold values from 0 to 163839, each once
- band_index: int32 [1], replicated, may hold values from 0 to 63
Outputs:
- learnability: float32 [2560], P('narrow')
- column_lse: float32 [2, 163840], P(None, ('wide', 'narrow'))
The draws below stay inside these ranges and needn't reach their ends.
Inputs may be any that keep to these rules, and one draw needn't show every extreme that they name: Text t is paired with image pair_ids[t], numbered band * 2560 + position in the band; every image has exactly one text.
All inputs are finite; a program needn't handle non-finite values.
Results may differ from the reference program's by a relative error of at most 0.0041.
Values may be sent and summed in bfloat16 or wider, within the bound.
No kernel may reach another device: no remote copies, remote signals or barrier semaphores. Data moves between devices by JAX's collectives and lax.ppermute only.
A program may use at most 128 MiB of HBM per device.

```python
import jax
import jax.numpy as jnp
from jax import lax

D_TOWER = 1024
D_EMB = 768
BAND = 2560
BANDS = 64
TEXTS = 163840
N_WIDE = 32


def tower_rows(key, count):
    base = jax.random.truncated_normal(jax.random.fold_in(key, 1), -5.0, 5.0, (count, D_TOWER), jnp.float32)
    rows = jnp.exp(jax.random.uniform(jax.random.fold_in(key, 2), (count, 1), jnp.float32, 0.0, 2.3026))
    cols = jnp.exp(jax.random.uniform(jax.random.fold_in(key, 3), (1, D_TOWER), jnp.float32, 0.0, 1.0986))
    return base * rows * cols


def image_rows(key):
    return tower_rows(jax.random.fold_in(key, 11), BANDS * BAND)


def draw_image_tower(key, part):
    return jnp.clip(image_rows(key), -150.0, 150.0).reshape(BANDS, BAND, D_TOWER).astype(jnp.bfloat16)


def draw_text_tower(key, part):
    texts = tower_rows(jax.random.fold_in(key, 12), TEXTS)
    return jnp.clip(texts, -150.0, 150.0).astype(jnp.bfloat16)


def head_weights(key, salt):
    values = jax.random.truncated_normal(jax.random.fold_in(key, salt), -5.0, 5.0, (2, D_TOWER, D_EMB), jnp.float32)
    return jnp.clip(values / jnp.sqrt(1.0 * D_TOWER), -1.0, 1.0)


def draw_image_proj(key, part):
    return head_weights(key, 21).astype(jnp.bfloat16)


def draw_text_proj(key, part):
    return head_weights(key, 22).astype(jnp.bfloat16)


def draw_logit_scale(key, part):
    return jax.random.uniform(jax.random.fold_in(key, 32), (2,), jnp.float32, 8.0, 30.0)


def setup_inputs(seed: int = 0) -> dict:
    key_list = jax.random.split(jax.random.key(seed), 8)
    image_tower = draw_image_tower(jax.random.fold_in(key_list[7], 71), 0)
    text_tower = draw_text_tower(jax.random.fold_in(key_list[7], 71), 0)
    image_proj = draw_image_proj(jax.random.fold_in(key_list[7], 71), 0)
    text_proj = draw_text_proj(jax.random.fold_in(key_list[7], 71), 0)
    logit_scale = draw_logit_scale(jax.random.fold_in(key_list[7], 71), 0)
    pair_ids = jax.random.permutation(key_list[5], TEXTS).astype(jnp.int32)
    band_index = jax.random.randint(key_list[6], (1,), 0, BANDS).astype(jnp.int32)
    return dict(image_tower=image_tower, text_tower=text_tower, image_proj=image_proj, text_proj=text_proj, logit_scale=logit_scale, pair_ids=pair_ids, band_index=band_index)


def embed(tower, weight):
    full = jnp.dot(tower.astype(jnp.float32), weight.astype(jnp.float32), precision=lax.Precision.HIGHEST)
    return (full * lax.rsqrt(lax.optimization_barrier(jnp.sum(full * full, axis=-1, keepdims=True)) + 1e-06)).astype(jnp.bfloat16)

def reference(image_tower, text_tower, image_proj, text_proj, logit_scale, pair_ids, band_index):
    start = band_index[0]
    band = lax.dynamic_index_in_dim(image_tower, start, 0, keepdims=False)
    img_emb = jnp.stack([embed(band, image_proj[0]), embed(band, image_proj[1])]).astype(jnp.float32)
    txt_emb = jnp.stack([embed(text_tower, text_proj[0]), embed(text_tower, text_proj[1])])
    block = TEXTS // N_WIDE
    blocks = TEXTS // block
    txt_blocks = txt_emb.reshape(2, blocks, block, D_EMB).transpose(1, 0, 2, 3)
    pair_blocks = pair_ids.reshape(blocks, block)
    target = (start * BAND + jnp.arange(BAND)).astype(jnp.int32)
    scale = logit_scale[:, None, None]

    def visit(carry, item):
        row_max, row_sum, row_pos = carry
        texts, pairs = item
        logits = scale * jnp.einsum('hid,hjd->hij', img_emb, texts.astype(jnp.float32), precision=lax.Precision.HIGHEST)
        col_max = lax.optimization_barrier(jnp.max(logits, axis=1))
        col_sum = lax.optimization_barrier(jnp.sum(jnp.exp(logits - col_max[:, None, :]), axis=1))
        new_max = jnp.maximum(row_max, lax.optimization_barrier(jnp.max(logits, axis=2)))
        row_sum = row_sum * jnp.exp(row_max - new_max) + lax.optimization_barrier(jnp.sum(jnp.exp(logits - new_max[:, :, None]), axis=2))
        hits = pairs[None, :] == target[:, None]
        row_pos = row_pos + lax.optimization_barrier(jnp.sum(jnp.where(hits[None], logits, 0.0), axis=2))
        return ((new_max, row_sum, row_pos), col_max + jnp.log(col_sum))
    init = (jnp.full((2, BAND), -1e+30, jnp.float32), jnp.zeros((2, BAND), jnp.float32), jnp.zeros((2, BAND), jnp.float32))
    (row_max, row_sum, row_pos), cols = lax.scan(visit, init, (txt_blocks, pair_blocks))
    losses = row_max + jnp.log(row_sum) - row_pos
    learnability = losses[0] - losses[1]
    column_lse = cols.transpose(1, 0, 2).reshape(2, TEXTS)
    return (learnability, column_lse)
```

```python
import functools

import jax
import jax.numpy as jnp
from jax import lax
from jax.experimental import pallas as pl
from jax.experimental.pallas import tpu as pltpu
from jax.sharding import Mesh
from jax.sharding import PartitionSpec as P

WIDE = ("z", "y", "xh")
NARROW = ("xl", "c")
ALL = WIDE + NARROW
X = ("xh", "xl")
PLANE = ("z", "y")
CHIPS = ("z", "y", "xh", "xl")


LOG2E = 1.4426950408889634
LN2 = 0.6931471805599453
LOW = -1e30
ROWS = 256
TILE = 256
A_ROWS = 24


def ring(step):
    return [(i, (i + step) % 4) for i in range(4)]


def from_ahead(value, axis):
    one = lax.ppermute(value, axis, ring(-1))
    three = lax.ppermute(value, axis, ring(1))
    two = lax.ppermute(value, axis, ring(2))
    return [value, one, two, three]


def text_kernel(x_ref, w_ref, o_ref):
    for h in range(2):
        f = jnp.dot(x_ref[...], w_ref[h], preferred_element_type=jnp.float32)
        r = lax.rsqrt(jnp.sum(f * f, axis=1, keepdims=True) + 1e-06)
        o_ref[h] = (f * r).T.astype(jnp.bfloat16)


def embed_texts(text_tower, weights):
    texts, depth = text_tower.shape
    width = weights.shape[2]
    return pl.pallas_call(
        text_kernel,
        grid=(texts // TILE,),
        in_specs=[
            pl.BlockSpec((TILE, depth), lambda i: (i, 0)),
            pl.BlockSpec((2, depth, width), lambda i: (0, 0, 0)),
        ],
        out_specs=pl.BlockSpec((2, width, TILE), lambda i: (0, 0, i)),
        out_shape=jax.ShapeDtypeStruct((2, width, texts), jnp.bfloat16),
        compiler_params=pltpu.CompilerParams(vmem_limit_bytes=24 * 1024 * 1024),
        cost_estimate=pl.CostEstimate(
            flops=4 * texts * depth * width, bytes_accessed=10 * 1024 * 1024, transcendentals=0
        ),
        name="embed_texts",
    )(text_tower, weights)


def main_kernel(
    steps, tiles,
    tgt_ref, dst_ref, scale_ref, x_ref, w_ref, ta_ref, tb_ref, pid_ref,
    row_ref, col_ref,
    emb, logits, rmax, rsum, pos, cnow, cmax, csum, tgt, stage,
):
    s = pl.program_id(0)
    refs = (ta_ref, tb_ref)
    groups = ROWS // 8

    def embed(h):
        e = jnp.dot(x_ref[...], w_ref[h], preferred_element_type=jnp.float32)
        r = lax.rsqrt(jnp.sum(e * e, axis=1, keepdims=True) + 1e-06)
        emb[...] = (e * r).astype(jnp.bfloat16)

    def first(h, j, src):
        k = src * tiles + j
        at = pl.ds(pl.multiple_of(j * TILE, TILE), TILE)
        lt = jnp.dot(emb[...], refs[src][h, :, at], preferred_element_type=jnp.float32)
        lt = lt * scale_ref[h]
        logits[h, k] = lt
        a, b = lt[:, :128], lt[:, 128:]
        rmax[h] = jnp.maximum(rmax[h], jnp.maximum(a, b))
        cnow[h, k] = jnp.max(lt.reshape(groups, 8, TILE), axis=0)
        t = tgt[...]
        pid = pid_ref[src, :, at]
        found = jnp.where(t == pid[:, :128], a, 0.0) + jnp.where(t == pid[:, 128:], b, 0.0)
        pos[...] = pos[...] + found if h == 0 else pos[...] - found

    def second(h, j, src):
        k = src * tiles + j
        lt = logits[h, k]
        old = cmax[h, k]
        new = jnp.maximum(old, cnow[h, k])
        m = rmax[h]
        rsum[h] += jnp.exp2(lt[:, :128] - m) + jnp.exp2(lt[:, 128:] - m)
        part = jnp.sum(jnp.exp2(lt.reshape(groups, 8, TILE) - new[None]), axis=0)
        csum[h, k] = csum[h, k] * jnp.exp2(old - new) + part
        cmax[h, k] = new

    def put(k, step, value):
        wide = jnp.broadcast_to(value, (ROWS, 128))
        for g in range(groups):
            at = pl.ds(pl.multiple_of(dst_ref[step * groups + g] * 8, 8), 8)
            stage[k, at, :] = wide[g * 8 : g * 8 + 8]

    def rows_done(h, step):
        m = jnp.max(rmax[h], axis=1, keepdims=True)
        total = jnp.sum(rsum[h] * jnp.exp2(rmax[h] - m), axis=1, keepdims=True)
        put(h, step, LN2 * m + jnp.log(total))

    def clear(h):
        rmax[h] = jnp.full((ROWS, 128), LOW, jnp.float32)

    @pl.when(s == 0)
    def _():
        cmax[...] = jnp.full(cmax.shape, LOW, jnp.float32)
        csum[...] = jnp.zeros(csum.shape, jnp.float32)

    lane = lax.broadcasted_iota(jnp.int32, (8, 128), 0)
    for g in range(groups):
        tgt[g * 8 : g * 8 + 8, :] = lane + tgt_ref[s * groups + g]
    pos[...] = jnp.zeros(pos.shape, jnp.float32)

    embed(0)
    clear(0)

    @pl.when(s == 0)
    def _():
        @pl.loop(0, tiles)
        def _(j):
            for src in range(2):
                first(0, j, src)

    @pl.when(s > 0)
    def _():
        rsum[1] = jnp.zeros((ROWS, 128), jnp.float32)

        @pl.loop(0, tiles)
        def _(j):
            for src in range(2):
                first(0, j, src)
                second(1, j, src)

        rows_done(1, s - 1)

    embed(1)
    clear(1)
    rsum[0] = jnp.zeros((ROWS, 128), jnp.float32)

    @pl.loop(0, tiles)
    def _(j):
        for src in range(2):
            first(1, j, src)
            second(0, j, src)

    rows_done(0, s)
    put(2, s, LN2 * jnp.sum(pos[...], axis=1, keepdims=True))

    @pl.when(s == steps - 1)
    def _():
        rsum[1] = jnp.zeros((ROWS, 128), jnp.float32)

        @pl.loop(0, tiles)
        def _(j):
            for src in range(2):
                second(1, j, src)

        rows_done(1, s)
        for k in range(3):
            for b in range(stage.shape[1] // 128):
                row_ref[k, b : b + 1, :] = stage[k, b * 128 : b * 128 + 128, :].T[:1]
        for h in range(2):
            for src in range(2):
                for j in range(tiles):
                    k = src * tiles + j
                    m = jnp.max(cmax[h, k], axis=0, keepdims=True)
                    total = jnp.sum(csum[h, k] * jnp.exp2(cmax[h, k] - m), axis=0, keepdims=True)
                    col_ref[h, src, :, j * TILE : j * TILE + TILE] = LN2 * m + jnp.log(total)


def score(tgt, dst, scale, images, weights, own, other, pair_ids):
    count, depth = images.shape
    width, texts = own.shape[1:]
    steps, tiles = count // ROWS, texts // TILE
    smem = pl.BlockSpec(memory_space=pltpu.SMEM)
    whole = lambda *shape: pl.BlockSpec(shape, lambda i: (0,) * len(shape))
    f32 = lambda *shape: pltpu.VMEM(shape, jnp.float32)
    return pl.pallas_call(
        functools.partial(main_kernel, steps, tiles),
        grid=(steps,),
        in_specs=[
            smem,
            smem,
            smem,
            pl.BlockSpec((ROWS, depth), lambda i: (i, 0)),
            whole(2, depth, width),
            whole(2, width, texts),
            whole(2, width, texts),
            whole(2, 1, texts),
        ],
        out_specs=[whole(3, count // 128, 128), whole(2, 2, 1, texts)],
        out_shape=[
            jax.ShapeDtypeStruct((3, count // 128, 128), jnp.float32),
            jax.ShapeDtypeStruct((2, 2, 1, texts), jnp.float32),
        ],
        scratch_shapes=[
            pltpu.VMEM((ROWS, width), jnp.bfloat16),
            f32(2, 2 * tiles, ROWS, TILE),
            f32(2, ROWS, 128),
            f32(2, ROWS, 128),
            f32(ROWS, 128),
            f32(2, 2 * tiles, 8, TILE),
            f32(2, 2 * tiles, 8, TILE),
            f32(2, 2 * tiles, 8, TILE),
            pltpu.VMEM((ROWS, 128), jnp.int32),
            f32(3, count, 128),
        ],
        compiler_params=pltpu.CompilerParams(
            dimension_semantics=("arbitrary",), vmem_limit_bytes=40 * 1024 * 1024
        ),
        cost_estimate=pl.CostEstimate(
            flops=4 * count * width * (depth + 2 * texts),
            bytes_accessed=16 * 1024 * 1024,
            transcendentals=8 * count * texts,
        ),
        name="score",
    )(tgt, dst, scale, images, weights, own, other, pair_ids)


def pick(parts, which):
    out = parts[0]
    for k in range(1, len(parts)):
        out = jnp.where(which == k, parts[k], out)
    return out


def per_device(image_tower, text_tower, image_proj, text_proj, logit_scale, pair_ids, band_index):
    held, rows, depth = image_tower.shape
    texts = text_tower.shape[0]
    chunk = rows // 16
    b_rows = chunk - A_ROWS
    picked = band_index[0]
    owner = picked // held
    root = owner // 2
    z, y, x, c = (lax.axis_index(a) for a in ("z", "y", X, "c"))

    own = embed_texts(text_tower, text_proj)
    swap = [(0, 1), (1, 0)]
    other = lax.ppermute(own, "c", swap)
    ids = pair_ids.reshape(1, 1, texts)
    ids = jnp.concatenate([ids, lax.ppermute(ids, "c", swap)])

    mine = lax.dynamic_index_in_dim(image_tower, picked % held, 0, keepdims=False)
    spread = lax.all_to_all(mine.reshape(16, chunk, depth), PLANE, 0, 0, tiled=True)
    piece = lax.dynamic_index_in_dim(spread, root, 0, keepdims=False)
    line = from_ahead(piece, X)
    pair = [pick(line, (2 * (owner % 2) + k - x) % 4) for k in range(2)]
    part_a = jnp.stack([p[:A_ROWS] for p in pair])
    part_b = jnp.stack([p[A_ROWS:] for p in pair])
    part_a = jnp.concatenate(from_ahead(part_a, "y")).reshape(-1, depth)
    part_b = jnp.concatenate(from_ahead(part_b, "z")).reshape(-1, depth)
    images = jnp.concatenate(from_ahead(part_a, "z") + from_ahead(part_b, "y"))

    ahead = jnp.arange(4, dtype=jnp.int32)
    at_z, at_y = (z + ahead) % 4, (y + ahead) % 4
    half = jnp.arange(2, dtype=jnp.int32)
    run = jnp.arange(chunk // 8, dtype=jnp.int32)
    n_a = A_ROWS // 8

    def spell(block, which):
        full = block[:, :, None, None] * (chunk // 8) + which[None, None, None, :]
        return jnp.broadcast_to(full, (4, 4, 2, len(which))).reshape(-1)

    run_all = jnp.concatenate(
        [spell(at_z[:, None] * 4 + at_y[None, :], run[:n_a]), spell(at_z[None, :] * 4 + at_y[:, None], run[n_a:])]
    )
    half_all = jnp.concatenate(
        [jnp.broadcast_to(half[:, None], (4, 4, 2, k)).reshape(-1) for k in (n_a, len(run) - n_a)]
    )
    dst = half_all * (rows // 8) + run_all
    tgt = picked * (4 * rows) + (2 * half_all + c) * rows + run_all * 8

    by_row, by_col = score(
        tgt, dst, logit_scale * LOG2E, images, image_proj, own, other, ids
    )

    mixed = lax.ppermute(by_col[:, 1, 0], "c", swap)
    column_lse = jnp.logaddexp(by_col[:, 0, 0], mixed)

    by_row = by_row.reshape(3, 2, rows).transpose(1, 0, 2)
    sent = jnp.broadcast_to(by_row[None], (32, 2, 3, rows)).reshape(64, 3, rows)
    got = lax.all_to_all(sent, CHIPS, 0, 0, tiled=True)
    top = jnp.max(got[:, :2], axis=0)
    lse = top + jnp.log(jnp.sum(jnp.exp(got[:, :2] - top), axis=0))
    learnability = lse[0] - lse[1] - jnp.sum(got[:, 2], axis=0)
    return learnability, column_lse


def solution(mesh):
    split = Mesh(mesh.devices.reshape(4, 4, 2, 2, 2), ALL)
    placed = (P(WIDE, NARROW, None), P(ALL, None), P(), P(), P(), P(ALL), P())
    return jax.shard_map(
        per_device,
        mesh=split,
        in_specs=placed,
        out_specs=(P(NARROW), P(None, ALL)),
        check_vma=False,
    )
```

```python
import functools

import jax
import jax.numpy as jnp
from jax import lax
from jax.experimental import pallas as pl
from jax.experimental.pallas import tpu as pltpu
from jax.sharding import Mesh
from jax.sharding import PartitionSpec as P

WIDE = ("z", "y", "xh")
NARROW = ("xl", "c")
ALL = WIDE + NARROW
X = ("xh", "xl")
PLANE = ("z", "y")
CHIPS = ("z", "y", "xh", "xl")


LOG2E = 1.4426950408889634
LN2 = 0.6931471805599453
LOW = -1e30
ROWS = 256
TILE = 256
A_ROWS = 24


def ring(step):
    return [(i, (i + step) % 4) for i in range(4)]


def from_ahead(value, axis):
    one = lax.ppermute(value, axis, ring(-1))
    three = lax.ppermute(value, axis, ring(1))
    two = lax.ppermute(value, axis, ring(2))
    return [value, one, two, three]


def normal(rows, weight):
    full = jnp.dot(rows, weight, preferred_element_type=jnp.float32)
    return full * lax.rsqrt(jnp.sum(full * full, axis=1, keepdims=True) + 1e-06)


def text_kernel(x_ref, w_ref, o_ref):
    for h in range(2):
        o_ref[h] = normal(x_ref[...], w_ref[h]).T.astype(jnp.bfloat16)


def embed_texts(text_tower, weights):
    texts, depth = text_tower.shape
    width = weights.shape[2]
    return pl.pallas_call(
        text_kernel,
        grid=(texts // TILE,),
        in_specs=[
            pl.BlockSpec((TILE, depth), lambda i: (i, 0)),
            pl.BlockSpec((2, depth, width), lambda i: (0, 0, 0)),
        ],
        out_specs=pl.BlockSpec((2, width, TILE), lambda i: (0, 0, i)),
        out_shape=jax.ShapeDtypeStruct((2, width, texts), jnp.bfloat16),
        compiler_params=pltpu.CompilerParams(vmem_limit_bytes=20 * 1024 * 1024),
        cost_estimate=pl.CostEstimate(
            flops=4 * texts * depth * width, bytes_accessed=10 * 1024 * 1024, transcendentals=0
        ),
        name="embed_texts",
    )(text_tower, weights)


def image_kernel(count, *refs):
    w_ref, o_ref = refs[count], refs[count + 1]
    at = 0
    for k in range(count):
        rows = refs[k].shape[0]
        for h in range(2):
            o_ref[h, at : at + rows, :] = normal(refs[k][...], w_ref[h]).astype(jnp.bfloat16)
        at += rows


def embed_images(pieces, weights):
    _, depth, width = weights.shape
    rows = sum(p.shape[0] for p in pieces)
    return pl.pallas_call(
        functools.partial(image_kernel, len(pieces)),
        out_shape=jax.ShapeDtypeStruct((2, rows, width), jnp.bfloat16),
        compiler_params=pltpu.CompilerParams(vmem_limit_bytes=16 * 1024 * 1024),
        cost_estimate=pl.CostEstimate(
            flops=4 * rows * depth * width, bytes_accessed=4 * 1024 * 1024, transcendentals=0
        ),
        name="embed_images",
    )(*pieces, weights)


def main_kernel(
    steps, tiles,
    tgt_ref, dst_ref, scale_ref, emb_ref, ta_ref, tb_ref, pid_ref,
    row_ref, col_ref,
    logits0, logits1, rmax0, rmax1, rsum0, rsum1, pos,
    cnow0, cnow1, cmax0, cmax1, csum0, csum1, tgt, stage,
):
    s = pl.program_id(0)
    refs = (ta_ref, tb_ref)
    logits, rmax, rsum = (logits0, logits1), (rmax0, rmax1), (rsum0, rsum1)
    cnow, cmax, csum = (cnow0, cnow1), (cmax0, cmax1), (csum0, csum1)
    groups = ROWS // 8
    here = pl.ds(pl.multiple_of(s * ROWS, ROWS), ROWS)

    def first(h, j, src):
        k = src * tiles + j
        at = pl.ds(pl.multiple_of(j * TILE, TILE), TILE)
        lt = jnp.dot(emb_ref[h, here, :], refs[src][h, :, at], preferred_element_type=jnp.float32)
        lt = lt * scale_ref[h]
        logits[h][k] = lt
        a, b = lt[:, :128], lt[:, 128:]
        rmax[h][...] = jnp.maximum(rmax[h][...], jnp.maximum(a, b))
        cnow[h][k] = jnp.max(lt.reshape(groups, 8, TILE), axis=0)
        t = tgt[...]
        pid = pid_ref[src, :, at]
        found = jnp.where(t == pid[:, :128], a, 0.0) + jnp.where(t == pid[:, 128:], b, 0.0)
        pos[...] = pos[...] + found if h == 0 else pos[...] - found

    def second(h, j, src):
        k = src * tiles + j
        lt = logits[h][k]
        old = cmax[h][k]
        new = jnp.maximum(old, cnow[h][k])
        m = rmax[h][...]
        rsum[h][...] += jnp.exp2(lt[:, :128] - m) + jnp.exp2(lt[:, 128:] - m)
        part = jnp.sum(jnp.exp2(lt.reshape(groups, 8, TILE) - new[None]), axis=0)
        csum[h][k] = csum[h][k] * jnp.exp2(old - new) + part
        cmax[h][k] = new

    def both(one, two):
        rmax[one][...] = jnp.full((ROWS, 128), LOW, jnp.float32)
        rsum[two][...] = jnp.zeros((ROWS, 128), jnp.float32)

        @pl.loop(0, tiles)
        def _(j):
            for src in range(2):
                second(two, j, src)
                first(one, j, src)

    def put(k, step, value):
        wide = jnp.broadcast_to(value, (ROWS, 128))
        for g in range(groups):
            at = pl.ds(pl.multiple_of(dst_ref[step * groups + g] * 8, 8), 8)
            stage[k, at, :] = wide[g * 8 : g * 8 + 8]

    def rows_done(h, step):
        m = jnp.max(rmax[h][...], axis=1, keepdims=True)
        total = jnp.sum(rsum[h][...] * jnp.exp2(rmax[h][...] - m), axis=1, keepdims=True)
        put(h, step, LN2 * m + jnp.log(total))

    def clear(h):
        cmax[h][...] = jnp.full(cmax[h].shape, LOW, jnp.float32)
        csum[h][...] = jnp.zeros(csum[h].shape, jnp.float32)

    def quick(h, j, src):
        k = src * tiles + j
        at = slice(j * TILE, j * TILE + TILE)
        lt = jnp.dot(emb_ref[h, here, :], refs[src][h, :, at], preferred_element_type=jnp.float32)
        lt = lt * scale_ref[h]
        e = jnp.exp2(lt)
        part = e[:, :128] + e[:, 128:]
        rsum[h][...] = rsum[h][...] + part if k else part
        csum[h][k] += jnp.sum(e.reshape(groups, 8, TILE), axis=0)
        t = tgt[...]
        pid = pid_ref[src, :, at]
        found = jnp.where(t == pid[:, :128], lt[:, :128], 0.0)
        found += jnp.where(t == pid[:, 128:], lt[:, 128:], 0.0)
        if h == 0:
            pos[...] = pos[...] + found if k else found
        else:
            pos[...] = pos[...] - found

    def write_rows():
        for k in range(3):
            for b in range(stage.shape[1] // 128):
                row_ref[k, b : b + 1, :] = stage[k, b * 128 : b * 128 + 128, :].T[:1]

    sub = lax.broadcasted_iota(jnp.int32, (8, 128), 0)
    for g in range(groups):
        tgt[g * 8 : g * 8 + 8, :] = sub + tgt_ref[s * groups + g]

    small = jnp.maximum(scale_ref[0], scale_ref[1]) * 1.01 < 114.0

    @pl.when(small)
    def _():
        @pl.when(s == 0)
        def _():
            for h in range(2):
                csum[h][...] = jnp.zeros(csum[h].shape, jnp.float32)

        for h in range(2):
            for src in range(2):
                for j in range(tiles):
                    quick(h, j, src)
        for h in range(2):
            put(h, s, jnp.log(jnp.sum(rsum[h][...], axis=1, keepdims=True)))
        put(2, s, LN2 * jnp.sum(pos[...], axis=1, keepdims=True))

        @pl.when(s == steps - 1)
        def _():
            write_rows()
            for h in range(2):
                for src in range(2):
                    for j in range(tiles):
                        total = jnp.sum(csum[h][src * tiles + j], axis=0, keepdims=True)
                        col_ref[h, src, :, j * TILE : j * TILE + TILE] = jnp.log(total)

    @pl.when(jnp.logical_not(small))
    def _():
        @pl.when(s == 0)
        def _():
            clear(0)
            logits1[...] = jnp.zeros(logits1.shape, jnp.float32)
            rmax1[...] = jnp.zeros(rmax1.shape, jnp.float32)
            cnow1[...] = jnp.zeros(cnow1.shape, jnp.float32)
            clear(1)

        pos[...] = jnp.zeros(pos.shape, jnp.float32)
        both(0, 1)

        @pl.when(s == 0)
        def _():
            clear(1)

        @pl.when(s > 0)
        def _():
            rows_done(1, s - 1)

        both(1, 0)
        rows_done(0, s)
        put(2, s, LN2 * jnp.sum(pos[...], axis=1, keepdims=True))

        @pl.when(s == steps - 1)
        def _():
            rsum[1][...] = jnp.zeros((ROWS, 128), jnp.float32)

            @pl.loop(0, tiles)
            def _(j):
                for src in range(2):
                    second(1, j, src)

            rows_done(1, s)
            write_rows()
            for h in range(2):
                for k in range(2 * tiles):
                    src, j = divmod(k, tiles)
                    m = jnp.max(cmax[h][k], axis=0, keepdims=True)
                    total = jnp.sum(csum[h][k] * jnp.exp2(cmax[h][k] - m), axis=0, keepdims=True)
                    col_ref[h, src, :, j * TILE : j * TILE + TILE] = LN2 * m + jnp.log(total)


def score(tgt, dst, scale, images, own, other, pair_ids):
    _, count, width = images.shape
    texts = own.shape[2]
    steps, tiles = count // ROWS, texts // TILE
    smem = pl.BlockSpec(memory_space=pltpu.SMEM)
    whole = lambda *shape: pl.BlockSpec(shape, lambda i: (0,) * len(shape))
    f32 = lambda *shape: pltpu.VMEM(shape, jnp.float32)
    twice = lambda ref: [ref, ref]
    return pl.pallas_call(
        functools.partial(main_kernel, steps, tiles),
        grid=(steps,),
        in_specs=[
            smem,
            smem,
            smem,
            whole(2, count, width),
            whole(2, width, texts),
            whole(2, width, texts),
            whole(2, 1, texts),
        ],
        out_specs=[whole(3, count // 128, 128), whole(2, 2, 1, texts)],
        out_shape=[
            jax.ShapeDtypeStruct((3, count // 128, 128), jnp.float32),
            jax.ShapeDtypeStruct((2, 2, 1, texts), jnp.float32),
        ],
        scratch_shapes=[
            *twice(f32(2 * tiles, ROWS, TILE)),
            *twice(f32(ROWS, 128)),
            *twice(f32(ROWS, 128)),
            f32(ROWS, 128),
            *twice(f32(2 * tiles, 8, TILE)),
            *twice(f32(2 * tiles, 8, TILE)),
            *twice(f32(2 * tiles, 8, TILE)),
            pltpu.VMEM((ROWS, 128), jnp.int32),
            f32(3, count, 128),
        ],
        compiler_params=pltpu.CompilerParams(
            dimension_semantics=("arbitrary",), vmem_limit_bytes=32 * 1024 * 1024
        ),
        cost_estimate=pl.CostEstimate(
            flops=8 * count * width * texts,
            bytes_accessed=16 * 1024 * 1024,
            transcendentals=8 * count * texts,
        ),
        name="score",
    )(tgt, dst, scale, images, own, other, pair_ids)


GROUPS = (
    (("a", 0), ("b", 0)),
    (("b", 1), ("b", 3), ("b", 2)),
    (("a", 1), ("a", 3)),
    (("a", 2),),
)


def run_table(runs):
    n_a = A_ROWS // 8
    table = []
    for group in GROUPS:
        for kind, k in group:
            for other in range(4):
                for half in range(2):
                    for run in range(n_a) if kind == "a" else range(n_a, runs):
                        table.append((k, other, half, run) if kind == "a" else (other, k, half, run))
    return tuple(zip(*table))


def pick(parts, which):
    out = parts[0]
    for k in range(1, len(parts)):
        out = jnp.where(which == k, parts[k], out)
    return out


def per_device(image_tower, text_tower, image_proj, text_proj, logit_scale, pair_ids, band_index):
    held, rows, depth = image_tower.shape
    texts = text_tower.shape[0]
    chunk = rows // 16
    b_rows = chunk - A_ROWS
    picked = band_index[0]
    owner = picked // held
    root = owner // 2
    z, y, x, c = (lax.axis_index(a) for a in ("z", "y", X, "c"))

    own = embed_texts(text_tower, text_proj)
    swap = [(0, 1), (1, 0)]
    other = lax.ppermute(own, "c", swap)
    ids = pair_ids.reshape(1, 1, texts)
    ids = jnp.concatenate([ids, lax.ppermute(ids, "c", swap)])

    mine = lax.dynamic_index_in_dim(image_tower, picked % held, 0, keepdims=False)
    spread = lax.all_to_all(mine.reshape(16, chunk, depth), PLANE, 0, 0, tiled=True)
    piece = lax.dynamic_index_in_dim(spread, root, 0, keepdims=False)
    line = from_ahead(piece, X)
    pair = [pick(line, (2 * (owner % 2) + k - x) % 4) for k in range(2)]
    part_a = jnp.stack([p[:A_ROWS] for p in pair])
    part_b = jnp.stack([p[A_ROWS:] for p in pair])
    part_a = jnp.concatenate(from_ahead(part_a, "y")).reshape(-1, depth)
    part_b = jnp.concatenate(from_ahead(part_b, "z")).reshape(-1, depth)
    all_a = from_ahead(part_a, "z")
    all_b = from_ahead(part_b, "y")
    pieces = {("a", k): p for k, p in enumerate(all_a)} | {("b", k): p for k, p in enumerate(all_b)}
    emb = jnp.concatenate([embed_images([pieces[k] for k in g], image_proj) for g in GROUPS], axis=1)

    dz, dy, half, run = (jnp.asarray(v, jnp.int32) for v in run_table(chunk // 8))
    run = ((z + dz) % 4 * 4 + (y + dy) % 4) * (chunk // 8) + run
    dst = half * (rows // 8) + run
    tgt = picked * (4 * rows) + (2 * half + c) * rows + run * 8

    by_row, by_col = score(tgt, dst, logit_scale * LOG2E, emb, own, other, ids)

    mixed = lax.ppermute(by_col[:, 1, 0], "c", swap)
    column_lse = jnp.logaddexp(by_col[:, 0, 0], mixed)

    by_row = by_row.reshape(3, 2, rows).transpose(1, 0, 2)
    sent = jnp.broadcast_to(by_row[None], (32, 2, 3, rows)).reshape(64, 3, rows)
    got = lax.all_to_all(sent, CHIPS, 0, 0, tiled=True)
    top = jnp.max(got[:, :2], axis=0)
    lse = top + jnp.log(jnp.sum(jnp.exp(got[:, :2] - top), axis=0))
    learnability = lse[0] - lse[1] - jnp.sum(got[:, 2], axis=0)
    return learnability, column_lse


def solution(mesh):
    split = Mesh(mesh.devices.reshape(4, 4, 2, 2, 2), ALL)
    placed = (P(WIDE, NARROW, None), P(ALL, None), P(), P(), P(), P(ALL), P())
    return jax.shard_map(
        per_device,
        mesh=split,
        in_specs=placed,
        out_specs=(P(NARROW), P(None, ALL)),
        check_vma=False,
    )
```

```python
import functools

import jax
import jax.numpy as jnp
from jax import lax
from jax.experimental import pallas as pl
from jax.experimental.pallas import tpu as pltpu
from jax.sharding import Mesh
from jax.sharding import PartitionSpec as P

WIDE = ("z", "y", "xh")
NARROW = ("xl", "c")
ALL = WIDE + NARROW
X = ("xh", "xl")
PLANE = ("z", "y")
CHIPS = ("z", "y", "xh", "xl")


LOG2E = 1.4426950408889634
LN2 = 0.6931471805599453
LOW = -1e30
ROWS = 256
TILE = 256


def ring(step):
    return [(i, (i + step) % 4) for i in range(4)]


def from_ahead(value, axis):
    one = lax.ppermute(value, axis, ring(-1))
    three = lax.ppermute(value, axis, ring(1))
    two = lax.ppermute(value, axis, ring(2))
    return [value, one, two, three]


def normal(rows, weight):
    full = jnp.dot(rows, weight, preferred_element_type=jnp.float32)
    return full * lax.rsqrt(jnp.sum(full * full, axis=1, keepdims=True) + 1e-06)


def text_kernel(x_ref, w_ref, o_ref):
    for h in range(2):
        o_ref[h] = normal(x_ref[...], w_ref[h]).T.astype(jnp.bfloat16)


def embed_texts(text_tower, weights):
    texts, depth = text_tower.shape
    width = weights.shape[2]
    return pl.pallas_call(
        text_kernel,
        grid=(texts // TILE,),
        in_specs=[
            pl.BlockSpec((TILE, depth), lambda i: (i, 0)),
            pl.BlockSpec((2, depth, width), lambda i: (0, 0, 0)),
        ],
        out_specs=pl.BlockSpec((2, width, TILE), lambda i: (0, 0, i)),
        out_shape=jax.ShapeDtypeStruct((2, width, texts), jnp.bfloat16),
        compiler_params=pltpu.CompilerParams(vmem_limit_bytes=60 * 1024 * 1024),
        cost_estimate=pl.CostEstimate(
            flops=4 * texts * depth * width, bytes_accessed=10 * 1024 * 1024, transcendentals=0
        ),
        name="embed_texts",
    )(text_tower, weights)


def heads(refs, w_ref, o_ref, at):
    for ref in refs:
        rows = ref.shape[0]
        for h in range(2):
            o_ref[h, at : at + rows, :] = normal(ref[...], w_ref[h]).astype(jnp.bfloat16)
        at += rows


def image_kernel(count, *refs):
    heads(refs[:count], refs[count], refs[count + 1], 0)


def embed_images(pieces, weights):
    _, depth, width = weights.shape
    rows = sum(p.shape[0] for p in pieces)
    return pl.pallas_call(
        functools.partial(image_kernel, len(pieces)),
        out_shape=jax.ShapeDtypeStruct((2, rows, width), jnp.bfloat16),
        compiler_params=pltpu.CompilerParams(vmem_limit_bytes=16 * 1024 * 1024),
        cost_estimate=pl.CostEstimate(
            flops=4 * rows * depth * width, bytes_accessed=4 * 1024 * 1024, transcendentals=0
        ),
        name="embed_images",
    )(*pieces, weights)


def main_kernel(
    steps, tiles, ready, late,
    tgt_ref, dst_ref, scale_ref, *rest,
):
    embs, pieces = rest[:ready], rest[ready : ready + late]
    (
        w_ref, own_ref, other_ref, pid_ref, row_ref, col_ref,
        emb_ref, text_ref, sems,
        logits0, logits1, rmax0, rmax1, rsum0, rsum1, pos,
        cnow0, cnow1, cmax0, cmax1, csum0, csum1, tgt, stage,
    ) = rest[ready + late :]
    s = pl.program_id(0)
    refs = (text_ref.at[0], text_ref.at[1])
    logits, rmax, rsum = (logits0, logits1), (rmax0, rmax1), (rsum0, rsum1)
    cnow, cmax, csum = (cnow0, cnow1), (cmax0, cmax1), (csum0, csum1)
    groups = ROWS // 8
    here = pl.ds(pl.multiple_of(s * ROWS, ROWS), ROWS)

    def text_copy(h, src):
        ref = (own_ref, other_ref)[src]
        return pltpu.make_async_copy(ref.at[h], text_ref.at[src, h], sems.at[src, h])

    @pl.when(s == 0)
    def _():
        for h in range(2):
            for src in range(2):
                text_copy(h, src).start()
        at = 0
        for e in embs:
            rows = e.shape[1]
            for h in range(2):
                emb_ref[h, at : at + rows, :] = e[h]
            at += rows
        heads(pieces, w_ref, emb_ref, at)
        for src in range(2):
            text_copy(0, src).wait()

    def first(h, j, src):
        k = src * tiles + j
        at = pl.ds(pl.multiple_of(j * TILE, TILE), TILE)
        lt = jnp.dot(emb_ref[h, here, :], refs[src][h, :, at], preferred_element_type=jnp.float32)
        lt = lt * scale_ref[h]
        logits[h][k] = lt
        a, b = lt[:, :128], lt[:, 128:]
        rmax[h][...] = jnp.maximum(rmax[h][...], jnp.maximum(a, b))
        cnow[h][k] = jnp.max(lt.reshape(groups, 8, TILE), axis=0)
        t = tgt[...]
        pid = pid_ref[src, :, at]
        found = jnp.where(t == pid[:, :128], a, 0.0) + jnp.where(t == pid[:, 128:], b, 0.0)
        pos[...] = pos[...] + found if h == 0 else pos[...] - found

    def second(h, j, src):
        k = src * tiles + j
        lt = logits[h][k]
        old = cmax[h][k]
        new = jnp.maximum(old, cnow[h][k])
        m = rmax[h][...]
        rsum[h][...] += jnp.exp2(lt[:, :128] - m) + jnp.exp2(lt[:, 128:] - m)
        part = jnp.sum(jnp.exp2(lt.reshape(groups, 8, TILE) - new[None]), axis=0)
        csum[h][k] = csum[h][k] * jnp.exp2(old - new) + part
        cmax[h][k] = new

    def both(one, two):
        rmax[one][...] = jnp.full((ROWS, 128), LOW, jnp.float32)
        rsum[two][...] = jnp.zeros((ROWS, 128), jnp.float32)

        @pl.loop(0, tiles)
        def _(j):
            for src in range(2):
                second(two, j, src)
                first(one, j, src)

    def put(k, step, value):
        wide = jnp.broadcast_to(value, (ROWS, 128))
        for g in range(groups):
            at = pl.ds(pl.multiple_of(dst_ref[step * groups + g] * 8, 8), 8)
            stage[k, at, :] = wide[g * 8 : g * 8 + 8]

    def rows_done(h, step):
        m = jnp.max(rmax[h][...], axis=1, keepdims=True)
        total = jnp.sum(rsum[h][...] * jnp.exp2(rmax[h][...] - m), axis=1, keepdims=True)
        put(h, step, LN2 * m + jnp.log(total))

    def clear(h):
        cmax[h][...] = jnp.full(cmax[h].shape, LOW, jnp.float32)
        csum[h][...] = jnp.zeros(csum[h].shape, jnp.float32)

    def quick(h, j, src):
        k = src * tiles + j
        at = slice(j * TILE, j * TILE + TILE)
        lt = jnp.dot(emb_ref[h, here, :], refs[src][h, :, at], preferred_element_type=jnp.float32)
        lt = lt * scale_ref[h]
        e = jnp.exp2(lt)
        part = e[:, :128] + e[:, 128:]
        rsum[h][...] = rsum[h][...] + part if k else part
        csum[h][k] += jnp.sum(e.reshape(groups, 8, TILE), axis=0)
        t = tgt[...]
        pid = pid_ref[src, :, at]
        found = jnp.where(t == pid[:, :128], lt[:, :128], 0.0)
        found += jnp.where(t == pid[:, 128:], lt[:, 128:], 0.0)
        if h == 0:
            pos[...] = pos[...] + found if k else found
        else:
            pos[...] = pos[...] - found

    def write_rows():
        half = stage.shape[1] // 256
        for k in range(3):
            for b in range(2 * half):
                at = k * half + b % half
                row_ref[b // half, at : at + 1, :] = stage[k, b * 128 : b * 128 + 128, :].T[:1]

    sub = lax.broadcasted_iota(jnp.int32, (8, 128), 0)
    for g in range(groups):
        tgt[g * 8 : g * 8 + 8, :] = sub + tgt_ref[s * groups + g]

    small = jnp.maximum(scale_ref[0], scale_ref[1]) * 1.01 < 114.0

    def quick_head(h):
        @pl.when(s == 0)
        def _():
            csum[h][...] = jnp.zeros(csum[h].shape, jnp.float32)

        for src in range(2):
            for j in range(tiles):
                quick(h, j, src)
        put(h, s, jnp.log(jnp.sum(rsum[h][...], axis=1, keepdims=True)))

    @pl.when(small)
    def _():
        quick_head(0)

    @pl.when(s == 0)
    def _():
        for src in range(2):
            text_copy(1, src).wait()

    @pl.when(small)
    def _():
        quick_head(1)
        put(2, s, LN2 * jnp.sum(pos[...], axis=1, keepdims=True))

        @pl.when(s == steps - 1)
        def _():
            write_rows()
            for h in range(2):
                for src in range(2):
                    for j in range(tiles):
                        total = jnp.sum(csum[h][src * tiles + j], axis=0, keepdims=True)
                        col_ref[h, src, :, j * TILE : j * TILE + TILE] = jnp.log(total)

    @pl.when(jnp.logical_not(small))
    def _():
        @pl.when(s == 0)
        def _():
            clear(0)
            logits1[...] = jnp.zeros(logits1.shape, jnp.float32)
            rmax1[...] = jnp.zeros(rmax1.shape, jnp.float32)
            cnow1[...] = jnp.zeros(cnow1.shape, jnp.float32)
            clear(1)

        pos[...] = jnp.zeros(pos.shape, jnp.float32)
        both(0, 1)

        @pl.when(s == 0)
        def _():
            clear(1)

        @pl.when(s > 0)
        def _():
            rows_done(1, s - 1)

        both(1, 0)
        rows_done(0, s)
        put(2, s, LN2 * jnp.sum(pos[...], axis=1, keepdims=True))

        @pl.when(s == steps - 1)
        def _():
            rsum[1][...] = jnp.zeros((ROWS, 128), jnp.float32)

            @pl.loop(0, tiles)
            def _(j):
                for src in range(2):
                    second(1, j, src)

            rows_done(1, s)
            write_rows()
            for h in range(2):
                for k in range(2 * tiles):
                    src, j = divmod(k, tiles)
                    m = jnp.max(cmax[h][k], axis=0, keepdims=True)
                    total = jnp.sum(csum[h][k] * jnp.exp2(cmax[h][k] - m), axis=0, keepdims=True)
                    col_ref[h, src, :, j * TILE : j * TILE + TILE] = LN2 * m + jnp.log(total)


def score(tgt, dst, scale, embs, pieces, weights, own, other, pair_ids):
    _, depth, width = weights.shape
    texts = own.shape[2]
    count = len(tgt) * 8
    steps, tiles = count // ROWS, texts // TILE
    smem = pl.BlockSpec(memory_space=pltpu.SMEM)
    hbm = pl.BlockSpec(memory_space=pl.ANY)
    whole = lambda *shape: pl.BlockSpec(shape, lambda i: (0,) * len(shape))
    f32 = lambda *shape: pltpu.VMEM(shape, jnp.float32)
    twice = lambda ref: [ref, ref]
    outs = [(2, 3 * count // 256, 128), (2, 2, 1, texts)]
    return pl.pallas_call(
        functools.partial(main_kernel, steps, tiles, len(embs), len(pieces)),
        grid=(steps,),
        in_specs=[
            smem,
            smem,
            smem,
            *(whole(*v.shape) for v in embs),
            *(whole(*v.shape) for v in pieces),
            whole(2, depth, width),
            hbm,
            hbm,
            whole(2, 1, texts),
        ],
        out_specs=[whole(*shape) for shape in outs],
        out_shape=[jax.ShapeDtypeStruct(shape, jnp.float32) for shape in outs],
        scratch_shapes=[
            pltpu.VMEM((2, count, width), jnp.bfloat16),
            pltpu.VMEM((2, 2, width, texts), jnp.bfloat16),
            pltpu.SemaphoreType.DMA((2, 2)),
            *twice(f32(2 * tiles, ROWS, TILE)),
            *twice(f32(ROWS, 128)),
            *twice(f32(ROWS, 128)),
            f32(ROWS, 128),
            *twice(f32(2 * tiles, 8, TILE)),
            *twice(f32(2 * tiles, 8, TILE)),
            *twice(f32(2 * tiles, 8, TILE)),
            pltpu.VMEM((ROWS, 128), jnp.int32),
            f32(3, count, 128),
        ],
        compiler_params=pltpu.CompilerParams(
            dimension_semantics=("arbitrary",), vmem_limit_bytes=44 * 1024 * 1024
        ),
        cost_estimate=pl.CostEstimate(
            flops=8 * count * width * texts,
            bytes_accessed=16 * 1024 * 1024,
            transcendentals=4 * count * texts,
        ),
        name="score",
    )(tgt, dst, scale, *embs, *pieces, weights, own, other, pair_ids)


GROUPS = (
    (("a", 0), ("b", 0)),
    (("a", 1), ("b", 1)),
    (("a", 3), ("b", 3)),
    (("a", 2), ("b", 2)),
)


def run_table(runs):
    table = []
    for group in GROUPS:
        for kind, k in group:
            for other in range(4):
                for run in range(runs):
                    table.append((k, other, 0, run) if kind == "a" else (other, k, 1, run))
    return tuple(zip(*table))


def take_kernel(at_ref, x_ref, o_ref):
    o_ref[...] = x_ref[at_ref[0]]


def take(parts, which):
    return pl.pallas_call(
        take_kernel,
        in_specs=[pl.BlockSpec(memory_space=pltpu.SMEM), pl.BlockSpec(memory_space=pltpu.VMEM)],
        out_specs=pl.BlockSpec(memory_space=pltpu.VMEM),
        out_shape=jax.ShapeDtypeStruct(parts.shape[1:], parts.dtype),
        compiler_params=pltpu.CompilerParams(vmem_limit_bytes=4 * 1024 * 1024),
        name="take",
    )(which[None], parts)


def pick(parts, which):
    out = parts[0]
    for k in range(1, len(parts)):
        out = jnp.where(which == k, parts[k], out)
    return out


def per_device(image_tower, text_tower, image_proj, text_proj, logit_scale, pair_ids, band_index):
    held, rows, depth = image_tower.shape
    texts = text_tower.shape[0]
    chunk = rows // 16
    picked = band_index[0]
    owner = picked // held
    root = owner // 2
    z, y, x, c = (lax.axis_index(a) for a in ("z", "y", X, "c"))

    own = embed_texts(text_tower, text_proj)
    swap = [(0, 1), (1, 0)]
    other = lax.ppermute(own, "c", swap)
    ids = pair_ids.reshape(1, 1, texts)
    ids = jnp.concatenate([ids, lax.ppermute(ids, "c", swap)])

    mine = lax.dynamic_index_in_dim(image_tower, picked % held, 0, keepdims=False)
    spread = lax.all_to_all(mine.reshape(16, chunk, depth), PLANE, 0, 0, tiled=True)
    piece = take(spread, root)
    line = from_ahead(piece, X)
    pair = [pick(line, (2 * (owner % 2) + k - x) % 4) for k in range(2)]
    part_a = jnp.concatenate(from_ahead(pair[0], "y"))
    part_b = jnp.concatenate(from_ahead(pair[1], "z"))
    all_a = from_ahead(part_a, "z")
    all_b = from_ahead(part_b, "y")
    pieces = {("a", k): p for k, p in enumerate(all_a)} | {("b", k): p for k, p in enumerate(all_b)}
    groups = [[pieces[k] for k in g] for g in GROUPS]
    embs = [embed_images(g, image_proj) for g in groups[:-1]]

    dz, dy, half, run = (jnp.asarray(v, jnp.int32) for v in run_table(chunk // 8))
    run = ((z + dz) % 4 * 4 + (y + dy) % 4) * (chunk // 8) + run
    dst = half * (rows // 8) + run
    tgt = picked * (4 * rows) + (2 * half + c) * rows + run * 8

    by_row, by_col = score(
        tgt, dst, logit_scale * LOG2E, embs, groups[-1], image_proj, own, other, ids
    )

    mixed = lax.ppermute(by_col[:, 1, 0], "c", swap)
    column_lse = jnp.logaddexp(by_col[:, 0, 0], mixed)

    lines = by_row.shape[1]
    sent = jnp.broadcast_to(by_row[None], (32, 2, lines, 128)).reshape(64, lines, 128)
    got = lax.all_to_all(sent, CHIPS, 0, 0, tiled=True)
    got = [got[:, k * lines // 3 : (k + 1) * lines // 3] for k in range(3)]
    lse = []
    for part in got[:2]:
        top = jnp.max(part, axis=0)
        lse.append(top + jnp.log(jnp.sum(jnp.exp(part - top), axis=0)))
    learnability = (lse[0] - lse[1] - jnp.sum(got[2], axis=0)).reshape(rows)
    return learnability, column_lse


def solution(mesh):
    split = Mesh(mesh.devices.reshape(4, 4, 2, 2, 2), ALL)
    placed = (P(WIDE, NARROW, None), P(ALL, None), P(), P(), P(), P(ALL), P())
    return jax.shard_map(
        per_device,
        mesh=split,
        in_specs=placed,
        out_specs=(P(NARROW), P(None, ALL)),
        check_vma=False,
    )
```
